32 devices in a mesh: groups: 2 (over x), grid: 4 (over y, core), orb: 4 (over z).
Axes of the slice: x: 2, y: 2, z: 4, core: 2. Of those that a mesh axis runs over, the one named last changes fastest.
Arguments:
- orbitals: float32 [32, 2, 128, 128, 128], P(('groups', 'orb'), None, 'grid'), parts along dimension 0, may hold values from -6 to 6
- v_local: float32 [256, 128, 128], P(('groups', 'grid')), parts along dimension 0, may hold values from -24 to 24
- occupations: float32 [32], P('groups'), parts along dimension 0, may hold values from 0.05 to 0.5
Outputs:
- orbitals_next: float32 [32, 2, 128, 128, 128], P(('groups', 'orb'), None, 'grid'), parts along dimension 0
The draws below stay inside these ranges and needn't reach their ends.
There are 2 independent parts, one for each index of `groups`. The reference program is written for one: setup_inputs(seed, part) draws one part's arguments, and reference() takes and returns one part's arrays. A program takes and returns all parts, laid end to end along the dimension named above; each array names one. Nothing has to cross between parts.
All inputs are finite; a program needn't handle non-finite values.
Results may differ from the reference program's by a relative error of at most 0.00035.
Values sent between devices are 32-bit elements; how exact they have to be, the bound alone decides.
A program may use at most 128 MiB of HBM per device.

```python
import math
import jax
import jax.numpy as jnp
from jax import lax

NX = 128
NY = 128
NZ = 128
ORB = 16


def block_levels(rng, dims, split, low, high):
    def one(dim, blocks):
        steps = jax.random.uniform(jax.random.fold_in(jax.random.fold_in(rng, 6), dim), (blocks,), jnp.float32, low / len(split), high / len(split))
        return jnp.repeat(jnp.exp(steps), dims[dim] // blocks).reshape((-1,) + (1,) * (len(dims) - dim - 1))

    factor_of = one(*split[0])
    for cut in split[1:]:
        factor_of = factor_of * one(*cut)
    return factor_of


def bell_draw(rng, shape, spread, reach, pieces=(), dtype=jnp.bfloat16):
    array = jax.random.normal(rng, shape, jnp.float32) * spread
    if len(pieces) > 0:
        array = block_levels(rng, shape, pieces, -0.22, 0.18) * array
    return jnp.clip(array, min=-reach, max=reach).astype(dtype)


def setup_inputs(seed: int = 0, part: int = 0) -> dict:
    splits = jax.random.split(jax.random.key(seed), 4)
    own_keys = jax.random.split(jax.random.fold_in(splits[3], part), 4)
    return {
        "orbitals": bell_draw(own_keys[0], (ORB, 2, NX, NY, NZ), 1.0, 6.0, ((0, 4), (2, 4)), jnp.float32),
        "v_local": bell_draw(own_keys[1], (NX, NY, NZ), 4.0, 24.0, ((0, 4),), jnp.float32),
        "occupations": jnp.clip(jnp.exp(jax.random.uniform(own_keys[2], (ORB,), jnp.float32, math.log(0.05), math.log(0.5))), 0.05, 0.5),
    }


TIME_STEP = 0.05
KINETIC_RATE = 0.1
HARTREE_SCALE = math.pi


def wave_squared(length):
    wavenumber = jnp.fft.fftfreq(length).astype(jnp.float32) * (2.0 * math.pi)
    return wavenumber * wavenumber


def reference(orbitals, v_local, occupations):
    waves = wave_squared(NX)[:, None, None] + wave_squared(NY)[None, :, None] + wave_squared(NZ)[None, None, :]
    kinetic_turn = -KINETIC_RATE * waves
    propagator = lax.complex(jnp.cos(kinetic_turn), jnp.sin(kinetic_turn))
    spectrum = jnp.fft.fftn(lax.complex(orbitals[:, 0], orbitals[:, 1]), axes=(1, 2, 3))
    evolved = jnp.fft.ifftn(spectrum * propagator[None], axes=(1, 2, 3))
    evolved_re = jnp.real(evolved)
    evolved_im = jnp.imag(evolved)
    density = jnp.sum(occupations[:, None, None, None] * (evolved_re * evolved_re + evolved_im * evolved_im), axis=0)
    anchor = waves <= 0.0
    kernel = jnp.where(anchor, 0.0, HARTREE_SCALE / jnp.where(anchor, 1.0, waves))
    hartree = jnp.real(jnp.fft.ifftn(jnp.fft.fftn(density) * kernel))
    phase_angle = TIME_STEP * (v_local + hartree)
    cosine = jnp.cos(phase_angle)[None]
    sine = jnp.sin(phase_angle)[None]
    out_re = evolved_re * cosine + evolved_im * sine
    out_im = evolved_im * cosine - evolved_re * sine
    return jnp.stack([out_re, out_im], 1).astype(jnp.float32)
```

```python
from functools import partial
import math

import jax
import jax.numpy as jnp
import ml_dtypes
import numpy as np
from jax import lax
from jax.experimental import pallas as pl
from jax.experimental.pallas import tpu as pltpu
from jax.sharding import PartitionSpec as P

TIME_STEP = 0.05
KINETIC_RATE = 0.1
HARTREE_SCALE = math.pi
HIGHEST = lax.Precision.HIGHEST
VMEM_LIMIT = 50 * 1024 * 1024


def wave_squared(length):
    ids = np.arange(length)
    signed = np.where(ids < (length + 1) // 2, ids, ids - length)
    return (2.0 * np.pi * signed / length) ** 2


def fourier(length, sign):
    ids = np.arange(length)
    return np.exp(sign * 2j * np.pi * ((ids[:, None] * ids[None, :]) % length) / length)


def kinetic_matrix(length):
    phase = np.exp(-1j * KINETIC_RATE * wave_squared(length))
    return (fourier(length, 1) / length * phase[None, :]) @ fourier(length, -1)


def left_block(matrix):
    return np.block([[matrix.real, -matrix.imag], [matrix.imag, matrix.real]])


def right_block(matrix):
    return np.block([[matrix.real, matrix.imag], [-matrix.imag, matrix.real]])


def split_const(table):
    table = np.asarray(table, np.float32)
    high = table.astype(ml_dtypes.bfloat16)
    low = (table - high.astype(np.float32)).astype(ml_dtypes.bfloat16)
    return np.stack([high, low])


def split(values):
    high = values.astype(jnp.bfloat16)
    low = (values - high.astype(jnp.float32)).astype(jnp.bfloat16)
    return high, low


def dot(left, right):
    return jnp.dot(left, right, preferred_element_type=jnp.float32)


def data_by_table(values, table):
    high, low = split(values)
    return dot(high, table[0]) + dot(high, table[1]) + dot(low, table[0])


def table_by_data(table, values):
    high, low = split(values)
    return dot(table[0], high) + dot(table[1], high) + dot(table[0], low)


def local_kernel(psi_ref, wz_ref, wy_ref, out_ref):
    _, _, bx, ny, nz = psi_ref.shape
    grid_count, _, _, vy, _ = out_ref.shape
    real_part = psi_ref[0, 0].reshape(bx * ny, nz)
    imag_part = psi_ref[0, 1].reshape(bx * ny, nz)
    turned = data_by_table(jnp.concatenate([real_part, imag_part], 1), wz_ref)
    columns = [
        jnp.concatenate(
            [turned[p * ny : (p + 1) * ny, :nz], turned[p * ny : (p + 1) * ny, nz:]], 0
        )
        for p in range(bx)
    ]
    rows = table_by_data(wy_ref, jnp.concatenate(columns, 1))
    for g in range(grid_count):
        for c in range(2):
            start = c * ny + g * vy
            for p in range(bx):
                out_ref[g, c, p] = rows[start : start + vy, p * nz : (p + 1) * nz]


def kinetic_local(orbitals, layer, grid_count, wz, wy):
    _, _, planes, ny, nz = orbitals.shape
    bx = min(4, planes)
    vy = ny // grid_count
    return pl.pallas_call(
        local_kernel,
        grid=(planes // bx,),
        in_specs=[
            pl.BlockSpec((1, 2, bx, ny, nz), lambda i: (layer, 0, i, 0, 0)),
            pl.BlockSpec(wz.shape, lambda i: (0, 0, 0)),
            pl.BlockSpec(wy.shape, lambda i: (0, 0, 0)),
        ],
        out_specs=pl.BlockSpec((grid_count, 2, bx, vy, nz), lambda i: (0, 0, i, 0, 0)),
        out_shape=jax.ShapeDtypeStruct((grid_count, 2, planes, vy, nz), jnp.float32),
        compiler_params=pltpu.CompilerParams(vmem_limit_bytes=VMEM_LIMIT),
        cost_estimate=pl.CostEstimate(
            flops=3 * 8 * planes * ny * nz * (ny + nz),
            bytes_accessed=16 * planes * ny * nz,
            transcendentals=0,
        ),
    )(orbitals, wz, wy)


def across_kernel(planes, first, weight_ref, psi_ref, wx_ref, *refs):
    if first:
        out_ref, density_ref = refs
    else:
        earlier_ref, out_ref, density_ref = refs
    depth, by, nz = psi_ref.shape
    columns = jnp.concatenate([psi_ref[:, j, :] for j in range(by)], 1)
    moved = table_by_data(wx_ref, columns)
    squares = moved * moved
    weight = weight_ref[0]
    for j in range(by):
        out_ref[:, j, :] = moved[:, j * nz : (j + 1) * nz]
    for h in range(depth // (2 * planes)):
        low = 2 * h * planes
        term = weight * (squares[low : low + planes] + squares[low + planes : low + 2 * planes])
        for j in range(by):
            value = term[:, j * nz : (j + 1) * nz]
            if not first:
                value = value + earlier_ref[h * planes : (h + 1) * planes, j, :]
            density_ref[h * planes : (h + 1) * planes, j, :] = value


def kinetic_across(received, weight, density, wx):
    grid_count, _, planes, vy, nz = received.shape
    depth = grid_count * 2 * planes
    by = min(8, vy)
    first = density is None
    block = pl.BlockSpec((depth, by, nz), lambda i: (0, i, 0))
    density_block = pl.BlockSpec((depth // 2, by, nz), lambda i: (0, i, 0))
    in_specs = [
        pl.BlockSpec(memory_space=pltpu.SMEM),
        block,
        pl.BlockSpec(wx.shape, lambda i: (0, 0, 0)),
    ]
    operands = [weight, received.reshape(depth, vy, nz), wx]
    if not first:
        in_specs.append(density_block)
        operands.append(density)
    moved, density = pl.pallas_call(
        partial(across_kernel, planes, first),
        grid=(vy // by,),
        in_specs=in_specs,
        out_specs=[block, density_block],
        out_shape=[
            jax.ShapeDtypeStruct((depth, vy, nz), jnp.float32),
            jax.ShapeDtypeStruct((depth // 2, vy, nz), jnp.float32),
        ],
        compiler_params=pltpu.CompilerParams(vmem_limit_bytes=VMEM_LIMIT),
        cost_estimate=pl.CostEstimate(
            flops=3 * 2 * depth * depth * vy * nz,
            bytes_accessed=12 * depth * vy * nz,
            transcendentals=0,
        ),
    )(*operands)
    return moved.reshape(grid_count, 2, planes, vy, nz), density


def rotate_kernel(layers, *refs):
    cos_ref, sin_ref = refs[layers], refs[layers + 1]
    out_ref = refs[layers + 2]
    grid_count, _, _, vy, _ = refs[0].shape
    for g in range(grid_count):
        band = slice(g * vy, (g + 1) * vy)
        cosine = cos_ref[:, band, :]
        sine = sin_ref[:, band, :]
        for l in range(layers):
            real_part = refs[l][g, 0]
            imag_part = refs[l][g, 1]
            out_ref[l, 0, :, band, :] = real_part * cosine + imag_part * sine
            out_ref[l, 1, :, band, :] = imag_part * cosine - real_part * sine


def rotate(returned, cosine, sine):
    layers = len(returned)
    grid_count, _, planes, vy, nz = returned[0].shape
    ny = grid_count * vy
    bx = min(4, planes)
    field_block = pl.BlockSpec((bx, ny, nz), lambda i: (i, 0, 0))
    return pl.pallas_call(
        partial(rotate_kernel, layers),
        grid=(planes // bx,),
        in_specs=[pl.BlockSpec((grid_count, 2, bx, vy, nz), lambda i: (0, 0, i, 0, 0))] * layers
        + [field_block, field_block],
        out_specs=pl.BlockSpec((layers, 2, bx, ny, nz), lambda i: (0, 0, i, 0, 0)),
        out_shape=jax.ShapeDtypeStruct((layers, 2, planes, ny, nz), jnp.float32),
        compiler_params=pltpu.CompilerParams(vmem_limit_bytes=VMEM_LIMIT),
    )(*returned, cosine, sine)


def table_of(matrix):
    return (np.asarray(matrix.real, np.float32), np.asarray(matrix.imag, np.float32))


def apply_along(values, table, axis):
    contracted = jnp.tensordot(values, table, axes=([axis], [0]), precision=HIGHEST)
    return jnp.moveaxis(contracted, -1, axis)


def complex_along(real_part, imag_part, matrix, axis):
    table_re, table_im = table_of(matrix)
    new_re = apply_along(real_part, table_re, axis) - apply_along(imag_part, table_im, axis)
    new_im = apply_along(real_part, table_im, axis) + apply_along(imag_part, table_re, axis)
    return (new_re, new_im)


def coulomb_kernel(squares_x, squares_y, squares_z):
    total = squares_x[:, None, None] + squares_y[None, :, None] + squares_z[None, None, :]
    anchor = total <= 0.0
    return jnp.where(anchor, 0.0, HARTREE_SCALE / jnp.where(anchor, 1.0, total))


def poisson_shared(density):
    width_x, _, count_z = density.shape
    span_count = lax.axis_size("grid") * lax.axis_size("orb")
    block_x = width_x // span_count
    forward_z = table_of(fourier(count_z, -1))
    real_part, imag_part = (apply_along(density, forward_z[0], 2), apply_along(density, forward_z[1], 2))
    real_part, imag_part = complex_along(real_part, imag_part, fourier(width_x, -1), 0)
    spread = lax.all_to_all(
        jnp.stack([real_part, imag_part], 0),
        ("grid", "orb"),
        split_axis=1,
        concat_axis=2,
        tiled=True,
    )
    count_y = spread.shape[2]
    real_part, imag_part = complex_along(spread[0], spread[1], fourier(count_y, -1), 1)
    start_x = lax.axis_index(("grid", "orb")) * block_x
    squares_x = lax.dynamic_slice_in_dim(
        jnp.asarray(wave_squared(width_x), jnp.float32), start_x, block_x, 0
    )
    kernel = coulomb_kernel(
        squares_x,
        np.asarray(wave_squared(count_y), np.float32),
        np.asarray(wave_squared(count_z), np.float32),
    )
    real_part, imag_part = complex_along(
        real_part * kernel, imag_part * kernel, fourier(count_y, 1) / count_y, 1
    )
    back = lax.all_to_all(
        jnp.stack([real_part, imag_part], 0),
        ("grid", "orb"),
        split_axis=2,
        concat_axis=1,
        tiled=True,
    )
    real_part, imag_part = complex_along(back[0], back[1], fourier(width_x, 1) / width_x, 0)
    inverse_z = table_of(fourier(count_z, 1) / count_z)
    return apply_along(real_part, inverse_z[0], 2) - apply_along(imag_part, inverse_z[1], 2)


def body(orbitals, v_local, occupations):
    layers, _, planes, count_y, count_z = orbitals.shape
    grid_count = lax.axis_size("grid")
    orb_count = lax.axis_size("orb")
    width_x = planes * grid_count
    share_y = count_y // (grid_count * orb_count)
    wz = jnp.asarray(split_const(right_block(kinetic_matrix(count_z))))
    wy = jnp.asarray(split_const(left_block(kinetic_matrix(count_y))))
    order = np.arange(2 * width_x).reshape(2, grid_count, planes).transpose(1, 0, 2).reshape(-1)
    wx = jnp.asarray(split_const(left_block(kinetic_matrix(width_x))[order][:, order]))
    weights = lax.dynamic_slice_in_dim(occupations, lax.axis_index("orb") * layers, layers, 0)
    exchange = partial(lax.all_to_all, axis_name="grid", split_axis=0, concat_axis=0, tiled=True)

    received = [
        exchange(kinetic_local(orbitals, layer, grid_count, wz, wy)) for layer in range(layers)
    ]
    density = None
    returned = []
    for layer in range(layers):
        moved, density = kinetic_across(
            received[layer], weights[layer : layer + 1], density, wx
        )
        returned.append(exchange(moved))
    share = lax.psum_scatter(density, "orb", scatter_dimension=1, tiled=True)
    share, returned[0] = lax.optimization_barrier((share, returned[0]))
    hartree_lines = poisson_shared(share)
    rows_back = lax.all_to_all(hartree_lines, "grid", split_axis=0, concat_axis=1, tiled=True)
    gathered = lax.all_gather(rows_back, "orb", axis=0, tiled=False)
    hartree = gathered.reshape(orb_count, planes, grid_count, share_y, count_z)
    hartree = hartree.transpose(1, 2, 0, 3, 4).reshape(planes, count_y, count_z)
    angle = TIME_STEP * (v_local + hartree)
    return rotate(returned, jnp.cos(angle), jnp.sin(angle))


def solution(mesh):
    return jax.shard_map(
        body,
        mesh=mesh,
        in_specs=(
            P(("groups", "orb"), None, "grid", None, None),
            P(("groups", "grid"), None, None),
            P("groups"),
        ),
        out_specs=P(("groups", "orb"), None, "grid", None, None),
        check_vma=False,
    )
```
